32 devices in a mesh: row: 8 (over y, x, core), col: 4 (over z).
Axes of the slice: x: 2, y: 2, z: 4, core: 2. Of those that a mesh axis runs over, the one named last changes fastest.
Arguments:
- right_side: float32 [5, 8, 4, 32, 128], P(None, 'row', 'col'), may hold values from -6 to 6
- diag_blocks: float32 [5, 8, 4, 128, 128], P(None, 'row', 'col'), may hold values from -1 to 2, as said below
- off_blocks: float32 [8, 4, 4, 8, 128, 128], P('row', 'col'), may hold values from -0.1875 to 0.1875
- slot_target: int32 [8, 4, 4, 8], P('row', 'col'), may hold values from 0 to 7
- slot_level: int32 [8, 4, 4, 8], P('row', 'col'), may hold values from 0 to 3, as said below
- slot_position: int32 [8, 4, 4, 8], P('row', 'col'), may hold values from 0 to 3
- slot_count: int32 [8, 4, 4], P('row', 'col'), may hold values from 1 to 8
Outputs:
- solution: float32 [5, 8, 4, 32, 128], P(None, 'row', 'col')
The draws below stay inside these ranges and needn't reach their ends.
Inputs may be any that keep to these rules, and one draw needn't show every extreme that they name: slot_level[..., m, s] is a level below the target level m + 1. slot_target names a row group. slot_position names a column group. `diag_blocks`: each diagonal block is lower triangular with its diagonal between 1 and 2 and strictly lower entries of size at most 1 / sqrt(128).
All inputs are finite; a program needn't handle non-finite values.
Results may differ from the reference program's by a relative error of at most 0.0001.
Values sent between devices are 32-bit elements; how exact they have to be, the bound alone decides.
A program may use at most 64 MiB of HBM per device.

```python
import math
import jax
import jax.numpy as jnp
from jax import lax

B = 128
NRHS = 32
LEVELS = 5
SLOTS = 8
GRID_ROWS = 8
GRID_COLS = 4


def draw_diag_blocks(key, part):
    first_key, second_key, third_key = jax.random.split(key, 3)
    shape_all = (LEVELS, GRID_ROWS, GRID_COLS, B, B)
    limit = 1.0 / math.sqrt(B)
    strict = jax.random.uniform(first_key, shape_all, jnp.float32, -limit, limit)
    main = jax.random.uniform(second_key, shape_all[:-1], jnp.float32, 1.0, 2.0)
    matrix = jnp.tril(strict, -1) + main[..., None] * jnp.eye(B, dtype=jnp.float32)
    return matrix.astype(jnp.float32)


def draw_slot_level(key, part):
    bounds = jnp.arange(1, LEVELS, dtype=jnp.int32)[None, None, :, None]
    raw_bits = jax.random.randint(key, (GRID_ROWS, GRID_COLS, LEVELS - 1, SLOTS), 0, 1 << 20, dtype=jnp.int32)
    return (raw_bits % bounds).astype(jnp.int32)


def with_ends(array, key, low, top_value):
    extent = array.shape
    index_at = [jax.random.randint(jax.random.fold_in(key, axis), (), 0, extent[axis]) for axis in range(len(extent))]
    array = array.at[tuple(index_at)].set(low)
    longest = extent.index(max(extent))
    index_at[longest] = (index_at[longest] + 1) % extent[longest]
    return array.at[tuple(index_at)].set(top_value)


def levels(rng, dims, cuts, smallest, top_value):
    gain = 1.0
    for dim, parts in cuts:
        heights = jax.random.uniform(jax.random.fold_in(jax.random.fold_in(rng, 6), dim), (parts,), jnp.float32, smallest / len(cuts), top_value / len(cuts))
        gain = gain * jnp.repeat(jnp.exp(heights), dims[dim] // parts).reshape((-1,) + (1,) * (len(dims) - 1 - dim))
    return gain


def noise(stream_key, extent, scale, most, pieces=(), held_as=jnp.bfloat16):
    drawn = jax.random.normal(stream_key, extent, jnp.float32) * scale
    if len(pieces) > 0:
        drawn = levels(stream_key, extent, pieces, -0.22, 0.18) * drawn
    return jnp.clip(drawn, min=-most, max=most).astype(held_as)


def setup_inputs(seed: int = 0) -> dict:
    splits = jax.random.split(jax.random.key(seed), 8)
    return {
        "right_side": noise(splits[0], (LEVELS, GRID_ROWS, GRID_COLS, NRHS, B), 1.0, 6.0, ((1, 8), (2, 4)), jnp.float32),
        "diag_blocks": draw_diag_blocks(jax.random.fold_in(splits[7], 71), 0),
        "off_blocks": noise(splits[2], (GRID_ROWS, GRID_COLS, LEVELS - 1, SLOTS, B, B), (B * SLOTS) ** -0.5, 0.1875, ((0, 8), (1, 4)), jnp.float32),
        "slot_target": with_ends(jax.random.randint(splits[3], (GRID_ROWS, GRID_COLS, LEVELS - 1, SLOTS), 0, GRID_ROWS), jax.random.fold_in(splits[3], 1), 0, GRID_ROWS - 1).astype(jnp.int32),
        "slot_level": draw_slot_level(jax.random.fold_in(splits[7], 71), 0),
        "slot_position": with_ends(jax.random.randint(splits[5], (GRID_ROWS, GRID_COLS, LEVELS - 1, SLOTS), 0, GRID_COLS), jax.random.fold_in(splits[5], 1), 0, GRID_COLS - 1).astype(jnp.int32),
        "slot_count": with_ends(jax.random.randint(splits[6], (GRID_ROWS, GRID_COLS, LEVELS - 1), 1, SLOTS + 1), jax.random.fold_in(splits[6], 1), 1, SLOTS).astype(jnp.int32),
    }


def solve_block(diagonal, right_rows):
    return jax.scipy.linalg.solve_triangular(diagonal, right_rows.T, lower=True).T

def reference(right_side, diag_blocks, off_blocks, slot_target, slot_level, slot_position, slot_count):
    solver = jax.vmap(jax.vmap(solve_block))
    solved = [solver(diag_blocks[0], right_side[0])]
    row_index = jnp.arange(GRID_ROWS, dtype=jnp.int32)[:, None, None]
    slot_ids = jnp.arange(SLOTS, dtype=jnp.int32)
    group_ids = jnp.arange(GRID_ROWS, dtype=jnp.int32)
    for level_now in range(1, LEVELS):
        source_tier = level_now - 1
        gathered = jnp.stack(solved)
        operands = gathered[slot_level[:, :, source_tier], row_index, slot_position[:, :, source_tier]]
        active = (slot_ids[None, None, :] < slot_count[:, :, source_tier:source_tier + 1]).astype(jnp.float32)
        products = jnp.einsum('rcsnb,rcsab->rcsna', operands, off_blocks[:, :, source_tier], precision=lax.Precision.HIGHEST)
        products = products * active[:, :, :, None, None]
        selector = (slot_target[:, :, source_tier][..., None] == group_ids).astype(jnp.float32)
        coupling = jnp.einsum('rcst,rcsna->tcna', selector, products, precision=lax.Precision.HIGHEST)
        solved.append(solver(diag_blocks[level_now], right_side[level_now] - coupling))
    return jnp.stack(solved)
```

```python
import functools

import jax
import jax.numpy as jnp
from jax import lax
from jax.experimental import pallas as pl
from jax.experimental.pallas import tpu as pltpu
from jax.sharding import PartitionSpec as P

F32 = jnp.float32
BF16 = jnp.bfloat16
SEED_BLOCK = 32
CHAINS = 1


def split_parts(value):
    high = value.astype(BF16)
    return high, (value - high.astype(F32)).astype(BF16)


def exact_dot(left, right):
    return jnp.dot(left, right, precision=lax.Precision.HIGHEST, preferred_element_type=F32)


def unit_upper_inverse(strict):
    size = strict.shape[0]
    row_ids = lax.broadcasted_iota(jnp.int32, (size, size), 0)
    col_ids = lax.broadcasted_iota(jnp.int32, (size, size), 1)
    eye = (row_ids == col_ids).astype(F32)
    width = min(SEED_BLOCK, size)
    power = jnp.where(row_ids // width == col_ids // width, -strict, 0.0)
    inverse = eye + power
    reach = 2
    while reach < width:
        power = exact_dot(power, power)
        inverse = inverse + exact_dot(inverse, power)
        reach *= 2
    while width < size:
        inside = row_ids // (2 * width) == col_ids // (2 * width)
        across = row_ids // width != col_ids // width
        corner = jnp.where(inside & across, strict, 0.0)
        inverse = inverse - exact_dot(exact_dot(inverse, corner), inverse)
        width *= 2
    return inverse


def kernel(
    rows, cols,
    rhs_hbm, diag_hbm, off_hbm, target, source, position, count,
    out_ref,
    rhs, diag, off, inverse_parts, scale, off_parts, landed, known, partial, arrived,
    load_sem, col_send, col_recv, row_send, row_recv,
):
    levels, nrhs, size = rhs.shape
    slots = off.shape[1]
    my_row, my_col = lax.axis_index("row"), lax.axis_index("col")
    part_rows = nrhs // CHAINS

    loads = [
        pltpu.make_async_copy(diag_hbm.at[0, 0, 0], diag.at[0], load_sem.at[0]),
        pltpu.make_async_copy(rhs_hbm.at[:, 0, 0], rhs, load_sem.at[1]),
        pltpu.make_async_copy(diag_hbm.at[1:, 0, 0], diag.at[1:], load_sem.at[2]),
    ]
    off_loads = [
        pltpu.make_async_copy(off_hbm.at[0, 0, step], off.at[step], load_sem.at[3 + step])
        for step in range(levels - 1)
    ]
    for load in loads + off_loads:
        load.start()

    barrier = pltpu.get_barrier_semaphore()
    for shift in range(1, cols):
        pl.semaphore_signal(
            barrier, inc=1, device_id={"col": lax.rem(my_col + shift, cols)},
            device_id_type=pl.DeviceIdType.MESH,
        )
    for shift in range(1, rows):
        pl.semaphore_signal(
            barrier, inc=1, device_id={"row": lax.rem(my_row + shift, rows)},
            device_id_type=pl.DeviceIdType.MESH,
        )

    def col_copy(step, part, shift):
        return pltpu.make_async_remote_copy(
            src_ref=landed.at[step, part, 0],
            dst_ref=landed.at[step, part, shift],
            send_sem=col_send.at[step, part, shift],
            recv_sem=col_recv.at[step, part, shift],
            device_id={"col": lax.rem(my_col + shift, cols)},
            device_id_type=pl.DeviceIdType.MESH,
        )

    def row_copy(step, part, shift):
        return pltpu.make_async_remote_copy(
            src_ref=partial.at[step, part, shift],
            dst_ref=arrived.at[step, part, shift],
            send_sem=row_send.at[step, part, shift],
            recv_sem=row_recv.at[step, part, shift],
            device_id={"row": lax.rem(my_row + shift, rows)},
            device_id_type=pl.DeviceIdType.MESH,
        )

    def invert(step):
        upper = diag[step].T
        row_ids = lax.broadcasted_iota(jnp.int32, (size, size), 0)
        col_ids = lax.broadcasted_iota(jnp.int32, (size, size), 1)
        inverse_main = 1.0 / jnp.sum(
            jnp.where(row_ids == col_ids, upper, 0.0), axis=0, keepdims=True
        )
        strict = jnp.where(row_ids < col_ids, upper, 0.0) * inverse_main
        high, low = split_parts(unit_upper_inverse(strict))
        inverse_parts[step, :, :size] = high
        inverse_parts[step, :, size:] = low
        scale[step] = jnp.broadcast_to(inverse_main, scale.shape[1:])

    def split_off(step):
        off_loads[step].wait()
        for slot in range(slots):
            high, low = split_parts(off[step, slot])
            off_parts[slot, :size, :] = high
            off_parts[slot, size:, :] = low

    def four_terms(full):
        return (full[:part_rows, :size] + full[part_rows:, size:]) + (
            full[:part_rows, size:] + full[part_rows:, :size]
        )

    def solve(step, part):
        span = pl.ds(part * part_rows, part_rows)
        reduced = rhs[step, span]
        if step > 0:
            coupling = partial[step - 1, part, 0]
            for shift in range(1, rows):
                row_copy(step - 1, part, shift).wait_recv()
                coupling = coupling + arrived[step - 1, part, shift]
            reduced = reduced - coupling
        high, low = split_parts(reduced * scale[step, :1])
        full = jnp.dot(
            jnp.concatenate([high, low], axis=0), inverse_parts[step],
            preferred_element_type=F32,
        )
        current = four_terms(full)
        if step + 1 < levels:
            landed[step, part, 0] = current
        out_ref[step, 0, 0, span] = current

    def send_cols(step, part):
        for shift in range(cols - 1, 0, -1):
            col_copy(step, part, shift).start()

    def collect(step, part):
        for shift in range(cols):
            if shift > 0:
                col_copy(step, part, shift).wait_recv()
            high, low = split_parts(landed[step, part, shift])
            column = lax.rem(my_col + cols - shift, cols)
            known[part, step, column, :part_rows] = high
            known[part, step, column, part_rows:] = low

    def products(step, part):
        held = []
        for slot in range(slots):
            operand = known[part, source[0, 0, step, slot], position[0, 0, step, slot]]
            full = lax.dot_general(
                operand, off_parts[slot], (((1,), (1,)), ((), ())), preferred_element_type=F32
            )
            held.append(four_terms(full))
        used = count[0, 0, step]
        for shift in range(rows):
            row = lax.rem(my_row + shift, rows)
            total = None
            for slot in range(slots):
                here = (target[0, 0, step, slot] == row) & (slot < used)
                term = held[slot] * jnp.where(here, 1.0, 0.0).astype(F32)
                total = term if total is None else total + term
            partial[step, part, shift] = total

    def send_rows(step, part):
        for shift in range(1, rows):
            row_copy(step, part, shift).start()

    loads[0].wait()
    invert(0)
    loads[1].wait()
    pl.semaphore_wait(barrier, rows + cols - 2)
    for step in range(levels):
        for part in range(CHAINS):
            solve(step, part)
            if step + 1 < levels:
                send_cols(step, part)
        if step + 1 < levels:
            split_off(step)
            for part in range(CHAINS):
                collect(step, part)
                products(step, part)
                send_rows(step, part)
            if step == 0:
                loads[2].wait()
            invert(step + 1)
    for step in range(levels - 1):
        for part in range(CHAINS):
            for shift in range(1, cols):
                col_copy(step, part, shift).wait_send()
            for shift in range(1, rows):
                row_copy(step, part, shift).wait_send()


def solution(mesh):
    rows, cols = mesh.shape["row"], mesh.shape["col"]

    def per_device(
        right_side, diag_blocks, off_blocks, slot_target, slot_level, slot_position, slot_count
    ):
        levels, nrhs, size = right_side.shape[0], right_side.shape[3], right_side.shape[4]
        slots = off_blocks.shape[3]
        steps, part_rows = levels - 1, nrhs // CHAINS
        anywhere = pl.BlockSpec(memory_space=pl.ANY)
        scalars = pl.BlockSpec(memory_space=pltpu.SMEM)
        return pl.pallas_call(
            functools.partial(kernel, rows, cols),
            out_shape=jax.ShapeDtypeStruct(right_side.shape, F32),
            in_specs=[anywhere] * 3 + [scalars] * 4,
            out_specs=pl.BlockSpec(memory_space=pltpu.VMEM),
            scratch_shapes=[
                pltpu.VMEM((levels, nrhs, size), F32),
                pltpu.VMEM((levels, size, size), F32),
                pltpu.VMEM((steps, slots, size, size), F32),
                pltpu.VMEM((levels, size, 2 * size), BF16),
                pltpu.VMEM((levels, 8, size), F32),
                pltpu.VMEM((slots, 2 * size, size), BF16),
                pltpu.VMEM((steps, CHAINS, cols, part_rows, size), F32),
                pltpu.VMEM((CHAINS, steps, cols, 2 * part_rows, size), BF16),
                pltpu.VMEM((steps, CHAINS, rows, part_rows, size), F32),
                pltpu.VMEM((steps, CHAINS, rows, part_rows, size), F32),
                pltpu.SemaphoreType.DMA((3 + steps,)),
                pltpu.SemaphoreType.DMA((steps, CHAINS, cols)),
                pltpu.SemaphoreType.DMA((steps, CHAINS, cols)),
                pltpu.SemaphoreType.DMA((steps, CHAINS, rows)),
                pltpu.SemaphoreType.DMA((steps, CHAINS, rows)),
            ],
            compiler_params=pltpu.CompilerParams(collective_id=0, has_side_effects=True),
            name="level_solve",
        )(
            right_side, diag_blocks, off_blocks,
            slot_target, slot_level, slot_position, slot_count,
        )

    return jax.shard_map(
        per_device,
        mesh=mesh,
        in_specs=(
            P(None, "row", "col", None, None),
            P(None, "row", "col", None, None),
            P("row", "col", None, None, None, None),
            P("row", "col", None, None),
            P("row", "col", None, None),
            P("row", "col", None, None),
            P("row", "col", None),
        ),
        out_specs=P(None, "row", "col", None, None),
        check_vma=False,
    )
```

```python
import functools

import jax
import jax.numpy as jnp
from jax import lax
from jax.experimental import pallas as pl
from jax.experimental.pallas import tpu as pltpu
from jax.sharding import PartitionSpec as P

F32 = jnp.float32
BF16 = jnp.bfloat16
SEED_BLOCK = 32
CHAINS = 2


def split_parts(value):
    high = value.astype(BF16)
    return high, (value - high.astype(F32)).astype(BF16)


def exact_dot(left, right):
    return jnp.dot(left, right, precision=lax.Precision.HIGHEST, preferred_element_type=F32)


def unit_upper_inverse(strict):
    size = strict.shape[0]
    row_ids = lax.broadcasted_iota(jnp.int32, (size, size), 0)
    col_ids = lax.broadcasted_iota(jnp.int32, (size, size), 1)
    eye = (row_ids == col_ids).astype(F32)
    width = min(SEED_BLOCK, size)
    power = jnp.where(row_ids // width == col_ids // width, -strict, 0.0)
    inverse = eye + power
    reach = 2
    while reach < width:
        power = exact_dot(power, power)
        inverse = inverse + exact_dot(inverse, power)
        reach *= 2
    while width < size:
        inside = row_ids // (2 * width) == col_ids // (2 * width)
        across = row_ids // width != col_ids // width
        corner = jnp.where(inside & across, strict, 0.0)
        inverse = inverse - exact_dot(exact_dot(inverse, corner), inverse)
        width *= 2
    return inverse


def kernel(
    rows, cols,
    rhs_hbm, diag_hbm, off_hbm, target_hbm, source_hbm, position_hbm, count_hbm,
    out_ref,
    rhs, diag, off, inverse_parts, scale, off_parts, landed, known, partial, arrived,
    target, source, position, count, weights,
    load_sem, index_sem, col_send, col_recv, row_send, row_recv,
):
    levels, nrhs, size = rhs.shape
    slots = off.shape[1]
    my_row, my_col = lax.axis_index("row"), lax.axis_index("col")
    part_rows = nrhs // CHAINS

    loads = [
        pltpu.make_async_copy(diag_hbm.at[0, 0, 0], diag.at[0], load_sem.at[0]),
        pltpu.make_async_copy(rhs_hbm.at[:, 0, 0], rhs, load_sem.at[1]),
        pltpu.make_async_copy(diag_hbm.at[1:, 0, 0], diag.at[1:], load_sem.at[2]),
    ]
    off_loads = [
        pltpu.make_async_copy(off_hbm.at[0, 0, step], off.at[step], load_sem.at[3 + step])
        for step in range(levels - 1)
    ]
    index_loads = [
        pltpu.make_async_copy(source_ref, held_ref, index_sem.at[i])
        for i, (source_ref, held_ref) in enumerate(
            [(target_hbm, target), (source_hbm, source), (position_hbm, position), (count_hbm, count)]
        )
    ]
    for load in loads + index_loads + off_loads:
        load.start()

    barrier = pltpu.get_barrier_semaphore()
    for shift in range(1, cols):
        pl.semaphore_signal(
            barrier, inc=1, device_id={"col": lax.rem(my_col + shift, cols)},
            device_id_type=pl.DeviceIdType.MESH,
        )
    for shift in range(1, rows):
        pl.semaphore_signal(
            barrier, inc=1, device_id={"row": lax.rem(my_row + shift, rows)},
            device_id_type=pl.DeviceIdType.MESH,
        )

    def col_copy(step, part, shift):
        return pltpu.make_async_remote_copy(
            src_ref=landed.at[step, part, 0],
            dst_ref=landed.at[step, part, shift],
            send_sem=col_send.at[step, part, shift],
            recv_sem=col_recv.at[step, part, shift],
            device_id={"col": lax.rem(my_col + shift, cols)},
            device_id_type=pl.DeviceIdType.MESH,
        )

    def row_copy(step, part, shift):
        return pltpu.make_async_remote_copy(
            src_ref=partial.at[step, part, shift],
            dst_ref=arrived.at[step, part, shift],
            send_sem=row_send.at[step, part, shift],
            recv_sem=row_recv.at[step, part, shift],
            device_id={"row": lax.rem(my_row + shift, rows)},
            device_id_type=pl.DeviceIdType.MESH,
        )

    def invert(step):
        upper = diag[step].T
        row_ids = lax.broadcasted_iota(jnp.int32, (size, size), 0)
        col_ids = lax.broadcasted_iota(jnp.int32, (size, size), 1)
        inverse_main = 1.0 / jnp.sum(
            jnp.where(row_ids == col_ids, upper, 0.0), axis=0, keepdims=True
        )
        strict = jnp.where(row_ids < col_ids, upper, 0.0) * inverse_main
        high, low = split_parts(unit_upper_inverse(strict))
        inverse_parts[step, :, :size] = high
        inverse_parts[step, :, size:] = low
        scale[step] = jnp.broadcast_to(inverse_main, scale.shape[1:])

    def split_off(step):
        off_loads[step].wait()
        for slot in range(slots):
            high, low = split_parts(off[step, slot])
            off_parts[slot, :size, :] = high
            off_parts[slot, size:, :] = low

    def four_terms(full):
        return (full[:part_rows, :size] + full[part_rows:, size:]) + (
            full[:part_rows, size:] + full[part_rows:, :size]
        )

    def solve(step, part):
        span = pl.ds(part * part_rows, part_rows)
        reduced = rhs[step, span]
        if step > 0:
            coupling = partial[step - 1, part, 0]
            for shift in range(1, rows):
                row_copy(step - 1, part, shift).wait_recv()
                coupling = coupling + arrived[step - 1, part, shift]
            reduced = reduced - coupling
        high, low = split_parts(reduced * scale[step, :1])
        full = jnp.dot(
            jnp.concatenate([high, low], axis=0), inverse_parts[step],
            preferred_element_type=F32,
        )
        current = four_terms(full)
        if step + 1 < levels:
            landed[step, part, 0] = current
        out_ref[step, 0, 0, span] = current

    def send_cols(step, part):
        for shift in range(cols - 1, 0, -1):
            col_copy(step, part, shift).start()

    def collect(step, part):
        for shift in range(cols):
            if shift > 0:
                col_copy(step, part, shift).wait_recv()
            high, low = split_parts(landed[step, part, shift])
            column = lax.rem(my_col + cols - shift, cols)
            known[part, step, column, :part_rows] = high
            known[part, step, column, part_rows:] = low

    def weigh(step):
        used = count[0, 0, step]
        for shift in range(rows):
            row = lax.rem(my_row + shift, rows)
            for slot in range(slots):
                here = (target[0, 0, step, slot] == row) & (slot < used)
                weights[shift, slot : slot + 1, :] = jnp.full(
                    (1, size), jnp.where(here, 1.0, 0.0), F32
                )

    def products(step, part):
        held = []
        for slot in range(slots):
            operand = known[part, source[0, 0, step, slot], position[0, 0, step, slot]]
            full = lax.dot_general(
                operand, off_parts[slot], (((1,), (1,)), ((), ())), preferred_element_type=F32
            )
            held.append(four_terms(full))
        for shift in range(rows - 1, -1, -1):
            total = None
            for slot in range(slots):
                term = held[slot] * weights[shift, slot : slot + 1, :]
                total = term if total is None else total + term
            partial[step, part, shift] = total
            if shift > 0:
                row_copy(step, part, shift).start()

    loads[0].wait()
    invert(0)
    loads[1].wait()
    pl.semaphore_wait(barrier, rows + cols - 2)
    for step in range(levels):
        for part in range(CHAINS):
            solve(step, part)
            if step + 1 < levels:
                send_cols(step, part)
        if step + 1 < levels:
            if step == 0:
                for load in index_loads:
                    load.wait()
            split_off(step)
            weigh(step)
            for part in range(CHAINS):
                collect(step, part)
                products(step, part)
            if step == 0:
                loads[2].wait()
            invert(step + 1)
    for step in range(levels - 1):
        for part in range(CHAINS):
            for shift in range(1, cols):
                col_copy(step, part, shift).wait_send()
            for shift in range(1, rows):
                row_copy(step, part, shift).wait_send()


def solution(mesh):
    rows, cols = mesh.shape["row"], mesh.shape["col"]

    def per_device(
        right_side, diag_blocks, off_blocks, slot_target, slot_level, slot_position, slot_count
    ):
        levels, nrhs, size = right_side.shape[0], right_side.shape[3], right_side.shape[4]
        slots = off_blocks.shape[3]
        steps, part_rows = levels - 1, nrhs // CHAINS
        anywhere = pl.BlockSpec(memory_space=pl.ANY)
        return pl.pallas_call(
            functools.partial(kernel, rows, cols),
            out_shape=jax.ShapeDtypeStruct(right_side.shape, F32),
            in_specs=[anywhere] * 7,
            out_specs=pl.BlockSpec(memory_space=pltpu.VMEM),
            scratch_shapes=[
                pltpu.VMEM((levels, nrhs, size), F32),
                pltpu.VMEM((levels, size, size), F32),
                pltpu.VMEM((steps, slots, size, size), F32),
                pltpu.VMEM((levels, size, 2 * size), BF16),
                pltpu.VMEM((levels, 8, size), F32),
                pltpu.VMEM((slots, 2 * size, size), BF16),
                pltpu.VMEM((steps, CHAINS, cols, part_rows, size), F32),
                pltpu.VMEM((CHAINS, steps, cols, 2 * part_rows, size), BF16),
                pltpu.VMEM((steps, CHAINS, rows, part_rows, size), F32),
                pltpu.VMEM((steps, CHAINS, rows, part_rows, size), F32),
                pltpu.SMEM(slot_target.shape, jnp.int32),
                pltpu.SMEM(slot_level.shape, jnp.int32),
                pltpu.SMEM(slot_position.shape, jnp.int32),
                pltpu.SMEM(slot_count.shape, jnp.int32),
                pltpu.VMEM((rows, slots, size), F32),
                pltpu.SemaphoreType.DMA((3 + steps,)),
                pltpu.SemaphoreType.DMA((4,)),
                pltpu.SemaphoreType.DMA((steps, CHAINS, cols)),
                pltpu.SemaphoreType.DMA((steps, CHAINS, cols)),
                pltpu.SemaphoreType.DMA((steps, CHAINS, rows)),
                pltpu.SemaphoreType.DMA((steps, CHAINS, rows)),
            ],
            compiler_params=pltpu.CompilerParams(collective_id=0, has_side_effects=True),
            name="level_solve",
        )(
            right_side, diag_blocks, off_blocks,
            slot_target, slot_level, slot_position, slot_count,
        )

    return jax.shard_map(
        per_device,
        mesh=mesh,
        in_specs=(
            P(None, "row", "col", None, None),
            P(None, "row", "col", None, None),
            P("row", "col", None, None, None, None),
            P("row", "col", None, None),
            P("row", "col", None, None),
            P("row", "col", None, None),
            P("row", "col", None),
        ),
        out_specs=P(None, "row", "col", None, None),
        check_vma=False,
    )
```
